8 devices in a mesh: replica: 2 (over z, y), data: 4 (over x, core).
Axes of the slice: x: 2, y: 2, z: 1, core: 2. Of those that a mesh axis runs over, the one named last changes fastest.
Arguments:
- x_seq: bfloat16 [256, 16, 2048], P(('replica', 'data'))
- dy_seq: float32 [256, 16, 2048], P(('replica', 'data'))
- w_stack: bfloat16 [2, 4096, 8192], replicated
- b_stack: float32 [2, 8192], replicated
Outputs:
- output 1: float32 [2, 4096, 8192], replicated
- output 2: float32 [2, 8192], replicated
- output 3: float32 [256, 16, 2048], P(('replica', 'data'))
All inputs are finite; a program needn't handle non-finite values.
Results may differ from the reference program's by a relative error of at most 0.0129304.
Values are sent between devices in bfloat16 or wider.
A program may use at most 1.75 GiB of HBM per device.

```python
import jax
import jax.numpy as jnp
from jax import lax

HIDDEN = 2048
LAYERS = 2
BATCH_DEV = 32
SEQ = 16
REPLICA = 2
DATA = 4


def setup_inputs(seed: int = 0) -> dict:
    shards = REPLICA * DATA
    batch_rows = BATCH_DEV * shards
    key_list = jax.random.split(jax.random.key(seed), 4)
    x_seq = jax.random.normal(key_list[0], (batch_rows, SEQ, HIDDEN), jnp.float32).astype(jnp.bfloat16)
    dy_seq = jax.random.normal(key_list[1], (batch_rows, SEQ, HIDDEN), jnp.float32)
    w_scale = 1.5 * (2 * HIDDEN) ** -0.5
    w_stack = (jax.random.normal(key_list[2], (LAYERS, 2 * HIDDEN, 4 * HIDDEN), jnp.float32) * w_scale).astype(jnp.bfloat16)
    gate_shift = jnp.concatenate([jnp.ones((2 * HIDDEN,), jnp.float32), jnp.zeros((HIDDEN,), jnp.float32), jnp.ones((HIDDEN,), jnp.float32)])
    b_stack = gate_shift + 0.5 * jax.random.normal(key_list[3], (LAYERS, 4 * HIDDEN), jnp.float32)
    return {'x_seq': x_seq, 'dy_seq': dy_seq, 'w_stack': w_stack, 'b_stack': b_stack}


def layer_forward(u_seq, w_layer, b_layer):
    batch_rows = u_seq.shape[1]

    def time_step(carry_state, u_step):
        h_prev, c_prev = carry_state
        z_all = jnp.dot(jnp.concatenate([u_step, h_prev], axis=-1), w_layer, preferred_element_type=jnp.float32) + b_layer
        z_i, z_f, z_g, z_o = jnp.split(z_all, 4, axis=-1)
        gate_i = jax.nn.sigmoid(z_i)
        gate_f = jax.nn.sigmoid(z_f)
        gate_g = jnp.tanh(z_g)
        gate_o = jax.nn.sigmoid(z_o)
        c_new = gate_f * c_prev + gate_i * gate_g
        tanh_c = jnp.tanh(c_new)
        h_new = (gate_o * tanh_c).astype(jnp.bfloat16)
        return (h_new, c_new), (h_new, c_new, tanh_c, gate_i, gate_f, gate_g, gate_o)

    init_state = (jnp.zeros((batch_rows, HIDDEN), jnp.bfloat16), jnp.zeros((batch_rows, HIDDEN), jnp.float32))
    return lax.scan(time_step, init_state, u_seq)[1]


def layer_backward(u_seq, w_layer, saved_acts, dh_seq):
    h_seq, c_seq, tanh_seq, i_seq, f_seq, g_seq, o_seq = saved_acts
    h_prev_seq = jnp.concatenate([jnp.zeros_like(h_seq[:1]), h_seq[:-1]], axis=0)
    c_prev_seq = jnp.concatenate([jnp.zeros_like(c_seq[:1]), c_seq[:-1]], axis=0)

    def time_step(carry_state, step_in):
        dh_rec, dc_next = carry_state
        dh_out, c_prev, tanh_c, gate_i, gate_f, gate_g, gate_o = step_in
        dh_tot = dh_out + dh_rec
        dc_cur = dc_next + dh_tot * gate_o * (1.0 - tanh_c * tanh_c)
        dz_all = jnp.concatenate([dc_cur * gate_g * gate_i * (1.0 - gate_i), dc_cur * c_prev * gate_f * (1.0 - gate_f), dc_cur * gate_i * (1.0 - gate_g * gate_g), dh_tot * tanh_c * gate_o * (1.0 - gate_o)], axis=-1)
        dz_low = dz_all.astype(jnp.bfloat16)
        du_all = jnp.dot(dz_low, w_layer.T, preferred_element_type=jnp.float32)
        return (du_all[:, HIDDEN:], dc_cur * gate_f), (dz_low, du_all[:, :HIDDEN], jnp.sum(dz_all, axis=0))

    init_state = (jnp.zeros_like(dh_seq[0]), jnp.zeros_like(dh_seq[0]))
    dz_seq, dx_seq, db_steps = lax.scan(time_step, init_state, (dh_seq, c_prev_seq, tanh_seq, i_seq, f_seq, g_seq, o_seq), reverse=True)[1]
    uh_seq = jnp.concatenate([u_seq, h_prev_seq], axis=-1)
    row_count = uh_seq.shape[0] * uh_seq.shape[1]
    dw_layer = jnp.dot(uh_seq.reshape(row_count, 2 * HIDDEN).T, dz_seq.reshape(row_count, 4 * HIDDEN), preferred_element_type=jnp.float32)
    return dw_layer, jnp.sum(db_steps, axis=0), dx_seq


def shard_grads(x_rows, dy_rows, w_stack, b_stack):
    u_first = jnp.swapaxes(x_rows, 0, 1)

    def fwd_layer(u_seq, layer_in):
        saved_acts = layer_forward(u_seq, layer_in[0], layer_in[1])
        return saved_acts[0], (u_seq, saved_acts)

    layer_inputs, layer_saved = lax.scan(fwd_layer, u_first, (w_stack, b_stack))[1]

    def bwd_layer(dh_seq, layer_in):
        dw_layer, db_layer, dx_seq = layer_backward(layer_in[1], layer_in[0], layer_in[2], dh_seq)
        return dx_seq, (dw_layer, db_layer)

    dx_seq, grads = lax.scan(bwd_layer, jnp.swapaxes(dy_rows, 0, 1), (w_stack, layer_inputs, layer_saved), reverse=True)
    return grads[0], grads[1], jnp.swapaxes(dx_seq, 0, 1)


def reference(x_seq, dy_seq, w_stack, b_stack):
    shards = REPLICA * DATA
    x_parts = x_seq.reshape(shards, BATCH_DEV, SEQ, HIDDEN)
    dy_parts = dy_seq.reshape(shards, BATCH_DEV, SEQ, HIDDEN)

    def add_shard(totals, shard_in):
        dw_all, db_all, dx_rows = shard_grads(shard_in[0], shard_in[1], w_stack, b_stack)
        dw_sum = totals[0] + dw_all.astype(jnp.bfloat16).astype(jnp.float32)
        db_sum = totals[1] + db_all.astype(jnp.bfloat16).astype(jnp.float32)
        return (dw_sum, db_sum), dx_rows

    init_totals = (jnp.zeros(w_stack.shape, jnp.float32), jnp.zeros(b_stack.shape, jnp.float32))
    totals, dx_parts = lax.scan(add_shard, init_totals, (x_parts, dy_parts))
    return totals[0], totals[1], dx_parts.reshape(x_seq.shape)
```

```python
import functools

import jax
import jax.numpy as jnp
from jax import lax
from jax.experimental import pallas as pl
from jax.experimental.pallas import tpu as pltpu
from jax.sharding import PartitionSpec as P


VMEM_BYTES = 67043328
BF16, F32 = jnp.bfloat16, jnp.float32


def dot(a, b):
    return jnp.dot(a, b, preferred_element_type=F32)


def forward_kernel(layer, rows, steps, in_blk, n_blk, u_hbm, win_ref, b_ref, w_hbm, acts_ref, h_hbm, ht_hbm, wt_hbm, wrec, zin, uh, c_scr, wt_buf, ht_buf, sem_w, sem_u, sem_o):
    hidden = uh.shape[1]
    n_in = 4 * hidden // in_blk
    cut = hidden // steps
    i = pl.program_id(0)
    part = hidden // 8

    def w_copy(k):
        return pltpu.make_async_copy(w_hbm.at[layer, pl.ds(hidden + k * part, part)], wrec.at[pl.ds(k * part, part)], sem_w.at[k])

    def wt_copy(t):
        return pltpu.make_async_copy(wt_buf, wt_hbm.at[:, pl.ds(pl.multiple_of(t * cut, cut), cut)], sem_o.at[0])

    @pl.when(i == 0)
    def _():
        u_copy = pltpu.make_async_copy(u_hbm, uh, sem_u)
        u_copy.start()
        for k in range(8):
            w_copy(k).start()
        u_copy.wait()

    @pl.when(i < n_in)
    def _():
        zin[:, pl.ds(pl.multiple_of(i * in_blk, in_blk), in_blk)] = dot(uh[...], win_ref[0]) + b_ref[...]

    def step(t, first):
        now = pl.ds(pl.multiple_of(t * rows, rows), rows)
        wt_buf[...] = wrec[pl.ds(pl.multiple_of(t * cut, cut), cut), :].T
        h_prev = None if first else uh[pl.ds(pl.multiple_of((t - 1) * rows, rows), rows), :]
        for n0 in range(0, hidden, n_blk):
            cols = pl.ds(n0, n_blk)
            z = []
            for g in range(4):
                gcols = pl.ds(g * hidden + n0, n_blk)
                zg = zin[now, gcols]
                z.append(zg if first else zg + dot(h_prev, wrec[:, gcols]))
            gate_i, gate_f, gate_g, gate_o = jax.nn.sigmoid(z[0]), jax.nn.sigmoid(z[1]), jnp.tanh(z[2]), jax.nn.sigmoid(z[3])
            c_new = gate_i * gate_g if first else gate_f * c_scr[:, cols] + gate_i * gate_g
            tanh_c = jnp.tanh(c_new)
            c_scr[:, cols] = c_new
            uh[now, cols] = (gate_o * tanh_c).astype(BF16)
            for k, a in enumerate((gate_i, gate_f, gate_g, gate_o, tanh_c, c_new)):
                acts_ref[k, :, cols] = a

    @pl.when(i == n_in)
    def _():
        for k in range(8):
            w_copy(k).wait()
        step(0, True)
        wt_copy(0).start()

    @pl.when(i > n_in)
    def _():
        t = i - n_in
        wt_copy(t - 1).wait()
        step(t, False)
        wt_copy(t).start()

    @pl.when(i == n_in + steps - 1)
    def _():
        h_copy = pltpu.make_async_copy(uh, h_hbm, sem_u)
        h_copy.start()
        for k in range(8):
            ht_buf[pl.ds(k * part, part), :] = uh[:, pl.ds(k * part, part)].T
        ht_copy = pltpu.make_async_copy(ht_buf, ht_hbm, sem_o.at[1])
        ht_copy.start()
        wt_copy(steps - 1).wait()
        h_copy.wait()
        ht_copy.wait()


def forward(layer, u, w_stack, b_stack, rows, steps):
    total, hidden = u.shape
    in_blk, n_blk = hidden // 4, hidden // 4
    n_in = 4 * hidden // in_blk
    t_of = lambda i: jnp.maximum(i - n_in, 0)
    k_of = lambda i: jnp.minimum(i, n_in - 1)
    return pl.pallas_call(
        functools.partial(forward_kernel, layer, rows, steps, in_blk, n_blk),
        grid=(n_in + steps,),
        in_specs=[
            pl.BlockSpec(memory_space=pl.ANY),
            pl.BlockSpec((1, hidden, in_blk), lambda i: (layer, 0, k_of(i))),
            pl.BlockSpec((1, in_blk), lambda i: (0, k_of(i))),
            pl.BlockSpec(memory_space=pl.ANY),
        ],
        out_specs=[
            pl.BlockSpec((6, rows, hidden), lambda i: (0, t_of(i), 0)),
            pl.BlockSpec(memory_space=pl.ANY),
            pl.BlockSpec(memory_space=pl.ANY),
            pl.BlockSpec(memory_space=pl.ANY),
        ],
        out_shape=[
            jax.ShapeDtypeStruct((6, total, hidden), F32),
            jax.ShapeDtypeStruct((total, hidden), BF16),
            jax.ShapeDtypeStruct((hidden, total), BF16),
            jax.ShapeDtypeStruct((4 * hidden, hidden), BF16),
        ],
        scratch_shapes=[
            pltpu.VMEM((hidden, 4 * hidden), BF16),
            pltpu.VMEM((total, 4 * hidden), F32),
            pltpu.VMEM((total, hidden), BF16),
            pltpu.VMEM((rows, hidden), F32),
            pltpu.VMEM((4 * hidden, hidden // steps), BF16),
            pltpu.VMEM((hidden, total), BF16),
            pltpu.SemaphoreType.DMA((8,)),
            pltpu.SemaphoreType.DMA,
            pltpu.SemaphoreType.DMA((2,)),
        ],
        compiler_params=pltpu.CompilerParams(dimension_semantics=("arbitrary",), vmem_limit_bytes=VMEM_BYTES),
        cost_estimate=pl.CostEstimate(flops=4 * total * hidden * 4 * hidden, bytes_accessed=4 * hidden * hidden * 4 * 3, transcendentals=0),
    )(u, w_stack, b_stack[layer][None], w_stack)


def backward_kernel(carried, rows, t_top, n_e, widths, n_blk, *refs):
    refs = list(refs)
    e_refs = [refs.pop(0) for _ in range(n_e)]
    acts_ref, cprev_ref = refs.pop(0), refs.pop(0)
    if carried:
        dz_in, fdc_in, db_in = refs.pop(0), refs.pop(0), refs.pop(0)
    wt_hbm = refs.pop(0)
    dz_ref = refs.pop(0)
    starts = [sum(widths[:k]) for k in range(len(widths))]
    chunk_refs = [refs.pop(0) for _ in widths]
    fdc_ref, db_ref, wt, dz_scr, sem_w = refs
    hidden = fdc_ref.shape[1]
    part = hidden // 8
    s = pl.program_id(0)
    t = t_top - s

    def w_copy(k):
        return pltpu.make_async_copy(wt_hbm.at[pl.ds(k * 4 * part, 4 * part)], wt.at[pl.ds(k * 4 * part, 4 * part)], sem_w.at[k])

    def step(first):
        new, old = lax.rem(s, 2), lax.rem(s + 1, 2)
        later = None if first else dz_scr[old]
        for n0 in range(0, hidden, n_blk):
            cols = pl.ds(n0, n_blk)
            gate_i, gate_f, gate_g, gate_o, tanh_c = (acts_ref[k, :, cols] for k in range(5))
            c_prev = jnp.where(t > 0, cprev_ref[0, :, cols], 0.0)
            dh = e_refs[0][:, cols]
            if n_e > 1:
                dh = jnp.where(t < 8, dh, e_refs[1][:, cols])
            if not first:
                dh = dh + dot(later, wt[:, cols])
            dc = dh * gate_o * (1.0 - tanh_c * tanh_c)
            if not first:
                dc = fdc_ref[:, cols] + dc
            fdc_ref[:, cols] = dc * gate_f
            dz = (
                dc * gate_g * gate_i * (1.0 - gate_i),
                dc * c_prev * gate_f * (1.0 - gate_f),
                dc * gate_i * (1.0 - gate_g * gate_g),
                dh * tanh_c * gate_o * (1.0 - gate_o),
            )
            for k in range(4):
                at = k * hidden + n0
                gcols = pl.ds(at, n_blk)
                low = dz[k].astype(BF16)
                dz_scr[new, :, gcols] = low
                dz_ref[:, gcols] = low
                for ref, start in zip(chunk_refs, starts):
                    if start <= at < start + ref.shape[1]:
                        ref[:, pl.ds(at - start, n_blk)] = low
                part_sum = dz[k][0:8]
                for q in range(8, rows, 8):
                    part_sum = part_sum + dz[k][q : q + 8]
                if first:
                    db_ref[:, gcols] = part_sum
                else:
                    db_ref[:, gcols] += part_sum

    @pl.when(s == 0)
    def _():
        for k in range(8):
            w_copy(k).start()
        if carried:
            dz_scr[1] = dz_in[...]
            fdc_ref[...] = fdc_in[...]
            db_ref[...] = db_in[...]
        else:
            step(True)
        for k in range(8):
            w_copy(k).wait()

    @pl.when(s >= (0 if carried else 1))
    def _():
        step(False)


def backward(e_parts, acts, w_t, rows, t_top, n_steps, widths, carry):
    total, hidden = acts.shape[1:]
    steps = total // rows
    n_e, n_blk = len(e_parts), hidden // 4
    out_rows = n_steps * rows
    half = steps // 2
    if n_e == 1:
        e_specs = [pl.BlockSpec((rows, hidden), lambda s: (t_top - s, 0))]
    else:
        e_specs = [
            pl.BlockSpec((rows, hidden), lambda s: (jnp.minimum(t_top - s, half - 1), 0)),
            pl.BlockSpec((rows, hidden), lambda s: (jnp.maximum(t_top - s - half, 0), 0)),
        ]
    in_specs = e_specs + [
        pl.BlockSpec((6, rows, hidden), lambda s: (0, t_top - s, 0)),
        pl.BlockSpec((1, rows, hidden), lambda s: (5, jnp.maximum(t_top - s - 1, 0), 0)),
    ]
    args = list(e_parts) + [acts, acts]
    if carry is not None:
        in_specs += [
            pl.BlockSpec((rows, 4 * hidden), lambda s: (0, 0)),
            pl.BlockSpec((rows, hidden), lambda s: (0, 0)),
            pl.BlockSpec((8, 4 * hidden), lambda s: (0, 0)),
        ]
        args += list(carry)
    in_specs.append(pl.BlockSpec(memory_space=pl.ANY))
    args.append(w_t)
    back = lambda s: (n_steps - 1 - s, 0)
    out_specs = [pl.BlockSpec((rows, 4 * hidden), back)]
    out_shape = [jax.ShapeDtypeStruct((out_rows, 4 * hidden), BF16)]
    for width in widths:
        out_specs.append(pl.BlockSpec((rows, width), back))
        out_shape.append(jax.ShapeDtypeStruct((out_rows, width), BF16))
    out_specs += [pl.BlockSpec((rows, hidden), lambda s: (0, 0)), pl.BlockSpec((8, 4 * hidden), lambda s: (0, 0))]
    out_shape += [jax.ShapeDtypeStruct((rows, hidden), F32), jax.ShapeDtypeStruct((8, 4 * hidden), F32)]
    outs = pl.pallas_call(
        functools.partial(backward_kernel, carry is not None, rows, t_top, n_e, widths, n_blk),
        grid=(n_steps,),
        in_specs=in_specs,
        out_specs=out_specs,
        out_shape=out_shape,
        scratch_shapes=[
            pltpu.VMEM((4 * hidden, hidden), BF16),
            pltpu.VMEM((2, rows, 4 * hidden), BF16),
            pltpu.SemaphoreType.DMA((8,)),
        ],
        compiler_params=pltpu.CompilerParams(dimension_semantics=("arbitrary",), vmem_limit_bytes=VMEM_BYTES),
        cost_estimate=pl.CostEstimate(flops=2 * out_rows * hidden * 4 * hidden, bytes_accessed=4 * hidden * hidden * 4, transcendentals=0),
    )(*args)
    return outs[0], outs[1 : 1 + len(widths)], outs[-2], outs[-1]


def weight_kernel(rows, n_piece, m_blk, aliased, core_ref, *refs):
    refs = list(refs)
    u_ref, h_ref = refs.pop(0), refs.pop(0)
    dz_refs = [refs.pop(0) for _ in range(n_piece)]
    if aliased:
        refs.pop(0)
    out_ref, send_ref, late = refs
    d, n_dev = pl.program_id(1), pl.num_programs(1)
    hidden = u_ref.shape[1]
    tall = dz_refs[0].shape[1]
    for k, ref in enumerate(dz_refs):
        skip = rows if k == 0 else 0
        late[pl.ds(k * tall + skip - rows, tall - skip), :] = ref[0, skip:, :]
    late[pl.ds(n_piece * tall - rows, rows), :] = jnp.zeros((rows, late.shape[1]), BF16)

    def share(m0):
        if m0 < hidden:
            total = dot(u_ref[0, pl.ds(m0, m_blk), 0:tall], dz_refs[0][0])
            for k in range(1, n_piece):
                total += dot(u_ref[0, pl.ds(m0, m_blk), k * tall : (k + 1) * tall], dz_refs[k][0])
        else:
            total = dot(h_ref[0, pl.ds(m0 - hidden, m_blk), :], late[...])
        return total.astype(BF16).astype(F32)

    @pl.when(d < n_dev - 1)
    def _():
        for m0 in range(0, 2 * hidden, m_blk):
            at = pl.ds(m0, m_blk)
            out_ref[0, at, :] = jnp.where(d == 0, 0.0, out_ref[0, at, :]) + share(m0)

    @pl.when(d == n_dev - 1)
    def _():
        for m0 in range(0, 2 * hidden, m_blk):
            at = pl.ds(m0, m_blk)
            low = (out_ref[0, at, :] + share(m0)).astype(BF16)
            out_ref[0, at, :] = low.astype(F32)
            send_ref[0, at, :] = low


def weight_grads(layer, col_blk, n_col, n_blk, core, u_all, h_all, dz_pieces, rows, out_shape, dw_acc):
    n_dev, hidden, total = u_all.shape
    tall = dz_pieces[0][0].shape[1]
    n_piece = len(dz_pieces)
    aliased = dw_acc is not None
    whole = pl.BlockSpec((1, hidden, total), lambda j, d, c: (d, 0, 0))
    in_specs = [whole, whole]
    for _, base in dz_pieces:
        in_specs.append(pl.BlockSpec((1, tall, n_blk), lambda j, d, c, base=base: (d, 0, base + 2 * j + c[0])))
    args = [core, u_all, h_all] + [a for a, _ in dz_pieces]
    aliases = {}
    if aliased:
        in_specs.append(pl.BlockSpec(memory_space=pl.ANY))
        aliases = {len(args): 0}
        args.append(dw_acc)
    return pl.pallas_call(
        functools.partial(weight_kernel, rows, n_piece, hidden // 4, aliased),
        grid_spec=pltpu.PrefetchScalarGridSpec(
            num_scalar_prefetch=1,
            grid=(n_col, n_dev),
            in_specs=in_specs,
            out_specs=[
                pl.BlockSpec((1, 2 * hidden, n_blk), lambda j, d, c: (layer, 0, col_blk + 2 * j + c[0])),
                pl.BlockSpec((1, 2 * hidden, n_blk), lambda j, d, c: (j, 0, 0)),
            ],
            scratch_shapes=[pltpu.VMEM((total, n_blk), BF16)],
        ),
        out_shape=[out_shape, jax.ShapeDtypeStruct((n_col, 2 * hidden, n_blk), BF16)],
        input_output_aliases=aliases,
        compiler_params=pltpu.CompilerParams(dimension_semantics=("arbitrary", "arbitrary"), vmem_limit_bytes=VMEM_BYTES),
        cost_estimate=pl.CostEstimate(flops=2 * n_dev * total * 2 * hidden * n_col * n_blk, bytes_accessed=n_col * 48 * 2**20, transcendentals=0),
    )(*args)


def widen_kernel(core_ref, recv_ref, dw_ref, out_ref):
    out_ref[...] = recv_ref[...].astype(F32)


def widen(layer, col_blk, core, recv, dw_acc):
    n_col, tall, n_blk = recv.shape
    m_blk = tall // 4
    return pl.pallas_call(
        widen_kernel,
        grid_spec=pltpu.PrefetchScalarGridSpec(
            num_scalar_prefetch=1,
            grid=(n_col, tall // m_blk),
            in_specs=[pl.BlockSpec((1, m_blk, n_blk), lambda j, m, c: (j, m, 0)), pl.BlockSpec(memory_space=pl.ANY)],
            out_specs=pl.BlockSpec((1, m_blk, n_blk), lambda j, m, c: (layer, m, col_blk + 2 * j + 1 - c[0])),
        ),
        out_shape=jax.ShapeDtypeStruct(dw_acc.shape, F32),
        input_output_aliases={2: 0},
        compiler_params=pltpu.CompilerParams(dimension_semantics=("arbitrary", "arbitrary")),
        cost_estimate=pl.CostEstimate(flops=n_col * tall * n_blk, bytes_accessed=6 * n_col * tall * n_blk, transcendentals=0),
    )(core, recv, dw_acc)


def transpose_kernel(a_ref, out_ref):
    out_ref[...] = a_ref[...].T


def transpose(a):
    tall, wide = a.shape
    blk = wide // 8
    return pl.pallas_call(
        transpose_kernel,
        grid=(8,),
        in_specs=[pl.BlockSpec((tall, blk), lambda k: (0, k))],
        out_specs=pl.BlockSpec((blk, tall), lambda k: (k, 0)),
        out_shape=jax.ShapeDtypeStruct((wide, tall), a.dtype),
        cost_estimate=pl.CostEstimate(flops=tall * wide, bytes_accessed=4 * tall * wide, transcendentals=0),
        name="transpose_x",
    )(a)


EARLY_WIDTHS = (1, 1, 1, 1)
LAST_WIDTHS = (1, 1, 1, 0.5, 0.5)


def solution(mesh):
    axes = ("replica", "data")
    n_data = mesh.shape["data"]
    swap = [(k, k ^ 1) for k in range(n_data)]

    def gather(a):
        return lax.all_gather(a, axes, axis=0, tiled=False)

    def body(x_loc, dy_loc, w_stack, b_stack):
        rows, steps, hidden = x_loc.shape
        total = rows * steps
        half = steps // 2
        n_blk = hidden // 4
        core = lax.rem(lax.axis_index("data"), 2).astype(jnp.int32)[None]
        dw_shape = jax.ShapeDtypeStruct(w_stack.shape, F32)
        early_widths = [int(hidden * w) for w in EARLY_WIDTHS]
        last_widths = [int(hidden * w) for w in LAST_WIDTHS]

        u_0 = jnp.swapaxes(x_loc, 0, 1).reshape(total, hidden)
        e_1 = jnp.swapaxes(dy_loc, 0, 1).reshape(total, hidden)
        x_all = gather(transpose(u_0))
        acts_0, u_1, h0_t, w_t0 = forward(0, u_0, w_stack, b_stack, rows, steps)
        h0_all = gather(h0_t)
        acts_1, _, h1_t, w_t1 = forward(1, u_1, w_stack, b_stack, rows, steps)
        h1_all = gather(h1_t)

        dz_late, _, fdc, db = backward([e_1], acts_1, w_t1, rows, steps - 1, half, (), None)
        late_all = gather(dz_late)
        dz_early, early, _, db_1 = backward([e_1], acts_1, w_t1, rows, half - 1, half, early_widths, (dz_late, fdc, db))
        early_all = [gather(a) for a in early]
        e_0 = [jnp.einsum("rg,hg->rh", dz, w_stack[1, :hidden], preferred_element_type=F32) for dz in (dz_early, dz_late)]
        dz_0, last, _, db_0 = backward(e_0, acts_0, w_t0, rows, steps - 1, steps, last_widths, None)
        last_all = [gather(a) for a in last]
        dx = jnp.einsum("rg,hg->rh", dz_0, w_stack[0, :hidden], preferred_element_type=F32)
        dx = jnp.swapaxes(dx.reshape(steps, rows, hidden), 0, 1)
        db_low = jnp.stack([jnp.sum(db_0, axis=0), jnp.sum(db_1, axis=0)]).astype(BF16).astype(F32)
        db_sum = lax.psum(db_low, axes)
        early_all[0], dx = lax.optimization_barrier((early_all[0], dx))

        jobs = []
        at = 0
        for k, width in enumerate(early_widths):
            jobs.append((1, at // n_blk, width, h0_all, h1_all, ((early_all[k], 0), (late_all, at // n_blk))))
            at += width
        at = 0
        for k, width in enumerate(last_widths):
            jobs.append((0, at // n_blk, width, x_all, h0_all, ((last_all[k], 0),)))
            at += width
        dw, waiting = None, None
        for layer, col, width, u_all, h_all, pieces in jobs:
            dw, own = weight_grads(layer, col, width // n_blk // 2, n_blk, core, u_all, h_all, pieces, rows, dw_shape, dw)
            other = lax.ppermute(own, "data", swap)
            if waiting is not None:
                dw = widen(waiting[0], waiting[1], core, waiting[2], dw)
            waiting = (layer, col, other)
        dw = widen(waiting[0], waiting[1], core, waiting[2], dw)
        return dw, db_sum, dx

    return jax.shard_map(body, mesh=mesh, in_specs=(P(axes), P(axes), P(), P()), out_specs=(P(), P(), P(axes)), check_vma=False)
```

```python
import functools

import jax
import jax.numpy as jnp
from jax import lax
from jax.experimental import pallas as pl
from jax.experimental.pallas import tpu as pltpu
from jax.sharding import PartitionSpec as P


VMEM_BYTES = 67043328
BF16, F32 = jnp.bfloat16, jnp.float32
FORWARD_REPEAT = (4, 2)
BACKWARD_REPEAT = (4, 3)
PIECES = {1: (2, 2), 0: (1.5, 1, 1, 0.5)}


def dot(a, b):
    return jnp.dot(a, b, preferred_element_type=F32)


def repeated_dot(a, b, repeat):
    rows = a.shape[0]
    many = dot(jnp.concatenate([a] * repeat, axis=0), b)
    out = many[:rows]
    for k in range(1, repeat):
        out = jnp.maximum(out, many[k * rows : (k + 1) * rows])
    return out


def forward_kernel(layer, rows, steps, in_blk, n_blk, repeat, u_hbm, win_ref, b_ref, w_hbm, acts_ref, h_hbm, ht_hbm, wt_hbm, wrec, zin, uh, c_scr, wt_buf, ht_buf, sem_w, sem_u, sem_o):
    hidden = uh.shape[1]
    n_in = 4 * hidden // in_blk
    cut = hidden // steps
    i = pl.program_id(0)
    part = hidden // 8

    def w_copy(k):
        return pltpu.make_async_copy(w_hbm.at[layer, pl.ds(hidden + k * part, part)], wrec.at[pl.ds(k * part, part)], sem_w.at[k])

    def wt_copy(t):
        return pltpu.make_async_copy(wt_buf, wt_hbm.at[t], sem_o.at[0])

    @pl.when(i == 0)
    def _():
        u_copy = pltpu.make_async_copy(u_hbm, uh, sem_u)
        u_copy.start()
        for k in range(8):
            w_copy(k).start()
        u_copy.wait()

    @pl.when(i < n_in)
    def _():
        zin[:, pl.ds(pl.multiple_of(i * in_blk, in_blk), in_blk)] = dot(uh[...], win_ref[0]) + b_ref[...]

    def step(t, first):
        now = pl.ds(pl.multiple_of(t * rows, rows), rows)
        wt_buf[...] = wrec[pl.ds(pl.multiple_of(t * cut, cut), cut), :].T
        h_prev = None if first else uh[pl.ds(pl.multiple_of((t - 1) * rows, rows), rows), :]
        for n0 in range(0, hidden, n_blk):
            cols = pl.ds(n0, n_blk)
            z = []
            for g in range(4):
                gcols = pl.ds(g * hidden + n0, n_blk)
                zg = zin[now, gcols]
                z.append(zg if first else zg + repeated_dot(h_prev, wrec[:, gcols], repeat))
            gate_i, gate_f, gate_g, gate_o = jax.nn.sigmoid(z[0]), jax.nn.sigmoid(z[1]), jnp.tanh(z[2]), jax.nn.sigmoid(z[3])
            c_new = gate_i * gate_g if first else gate_f * c_scr[:, cols] + gate_i * gate_g
            tanh_c = jnp.tanh(c_new)
            c_scr[:, cols] = c_new
            uh[now, cols] = (gate_o * tanh_c).astype(BF16)
            for k, a in enumerate((gate_i, gate_f, gate_g, gate_o, tanh_c, c_new)):
                acts_ref[k, :, cols] = a

    @pl.when(i == n_in)
    def _():
        for k in range(8):
            w_copy(k).wait()
        step(0, True)
        wt_copy(0).start()

    @pl.when(i > n_in)
    def _():
        t = i - n_in
        wt_copy(t - 1).wait()
        step(t, False)
        wt_copy(t).start()

    @pl.when(i == n_in + steps - 1)
    def _():
        h_copy = pltpu.make_async_copy(uh, h_hbm, sem_u)
        h_copy.start()
        for k in range(8):
            ht_buf[pl.ds(k * part, part), :] = uh[:, pl.ds(k * part, part)].T
        ht_copy = pltpu.make_async_copy(ht_buf, ht_hbm, sem_o.at[1])
        ht_copy.start()
        wt_copy(steps - 1).wait()
        h_copy.wait()
        ht_copy.wait()


def forward(layer, u, w_stack, b_stack, rows, steps):
    total, hidden = u.shape
    in_blk, n_blk = hidden // 4, hidden // 4
    n_in = 4 * hidden // in_blk
    t_of = lambda i: jnp.maximum(i - n_in, 0)
    k_of = lambda i: jnp.minimum(i, n_in - 1)
    return pl.pallas_call(
        functools.partial(forward_kernel, layer, rows, steps, in_blk, n_blk, FORWARD_REPEAT[layer]),
        grid=(n_in + steps,),
        in_specs=[
            pl.BlockSpec(memory_space=pl.ANY),
            pl.BlockSpec((1, hidden, in_blk), lambda i: (layer, 0, k_of(i))),
            pl.BlockSpec((1, in_blk), lambda i: (0, k_of(i))),
            pl.BlockSpec(memory_space=pl.ANY),
        ],
        out_specs=[
            pl.BlockSpec((6, rows, hidden), lambda i: (0, t_of(i), 0)),
            pl.BlockSpec(memory_space=pl.ANY),
            pl.BlockSpec(memory_space=pl.ANY),
            pl.BlockSpec(memory_space=pl.ANY),
        ],
        out_shape=[
            jax.ShapeDtypeStruct((6, total, hidden), F32),
            jax.ShapeDtypeStruct((total, hidden), BF16),
            jax.ShapeDtypeStruct((hidden, total), BF16),
            jax.ShapeDtypeStruct((steps, 4 * hidden, hidden // steps), BF16),
        ],
        scratch_shapes=[
            pltpu.VMEM((hidden, 4 * hidden), BF16),
            pltpu.VMEM((total, 4 * hidden), F32),
            pltpu.VMEM((total, hidden), BF16),
            pltpu.VMEM((rows, hidden), F32),
            pltpu.VMEM((4 * hidden, hidden // steps), BF16),
            pltpu.VMEM((hidden, total), BF16),
            pltpu.SemaphoreType.DMA((8,)),
            pltpu.SemaphoreType.DMA,
            pltpu.SemaphoreType.DMA((2,)),
        ],
        compiler_params=pltpu.CompilerParams(dimension_semantics=("arbitrary",), vmem_limit_bytes=VMEM_BYTES),
        cost_estimate=pl.CostEstimate(flops=4 * total * hidden * 4 * hidden, bytes_accessed=4 * hidden * hidden * 4 * 3, transcendentals=0),
    )(u, w_stack, b_stack[layer][None], w_stack)


def backward_kernel(rows, n_steps, widths, n_blk, repeat, e_ref, acts_ref, cprev_ref, wt_hbm, dz_ref, *refs):
    piece_refs = refs[: len(widths)]
    db_ref, fdc, wt, dz_scr, sem_w = refs[len(widths) :]
    starts = [sum(widths[:k]) for k in range(len(widths))]
    hidden = fdc.shape[1]
    n_slab, _, cut = wt.shape
    s = pl.program_id(0)
    t = n_steps - 1 - s

    def w_copy(k):
        return pltpu.make_async_copy(wt_hbm.at[k], wt.at[k], sem_w.at[k])

    def step(first):
        new, old = lax.rem(s, 2), lax.rem(s + 1, 2)
        later = None if first else dz_scr[old]
        for n0 in range(0, hidden, n_blk):
            cols = pl.ds(n0, n_blk)
            gate_i, gate_f, gate_g, gate_o, tanh_c = (acts_ref[k, :, cols] for k in range(5))
            c_prev = jnp.where(t > 0, cprev_ref[0, :, cols], 0.0)
            dh = e_ref[:, cols]
            if not first:
                w_cols = jnp.concatenate([wt[n0 // cut + k] for k in range(n_blk // cut)], axis=1)
                dh = dh + repeated_dot(later, w_cols, repeat)
            dc = dh * gate_o * (1.0 - tanh_c * tanh_c)
            if not first:
                dc = fdc[:, cols] + dc
            fdc[:, cols] = dc * gate_f
            dz = (
                dc * gate_g * gate_i * (1.0 - gate_i),
                dc * c_prev * gate_f * (1.0 - gate_f),
                dc * gate_i * (1.0 - gate_g * gate_g),
                dh * tanh_c * gate_o * (1.0 - gate_o),
            )
            for k in range(4):
                at = k * hidden + n0
                gcols = pl.ds(at, n_blk)
                low = dz[k].astype(BF16)
                dz_scr[new, :, gcols] = low
                dz_ref[:, gcols] = low
                for ref, start in zip(piece_refs, starts):
                    if start <= at < start + ref.shape[1]:
                        ref[:, pl.ds(at - start, n_blk)] = low
                part_sum = dz[k][0:8]
                for q in range(8, rows, 8):
                    part_sum = part_sum + dz[k][q : q + 8]
                if first:
                    db_ref[:, gcols] = part_sum
                else:
                    db_ref[:, gcols] += part_sum

    @pl.when(s == 0)
    def _():
        for k in range(n_slab):
            w_copy(k).start()
        step(True)
        for k in range(n_slab):
            w_copy(k).wait()

    @pl.when(s > 0)
    def _():
        step(False)


def backward(layer, e, acts, w_t, rows, widths):
    total, hidden = acts.shape[1:]
    steps = total // rows
    back = lambda s: (steps - 1 - s, 0)
    outs = pl.pallas_call(
        functools.partial(backward_kernel, rows, steps, widths, hidden // 8, BACKWARD_REPEAT[layer]),
        grid=(steps,),
        in_specs=[
            pl.BlockSpec((rows, hidden), back),
            pl.BlockSpec((6, rows, hidden), lambda s: (0, steps - 1 - s, 0)),
            pl.BlockSpec((1, rows, hidden), lambda s: (5, jnp.maximum(steps - 2 - s, 0), 0)),
            pl.BlockSpec(memory_space=pl.ANY),
        ],
        out_specs=[pl.BlockSpec((rows, w), back) for w in (4 * hidden, *widths)] + [pl.BlockSpec((8, 4 * hidden), lambda s: (0, 0))],
        out_shape=[jax.ShapeDtypeStruct((total, w), BF16) for w in (4 * hidden, *widths)] + [jax.ShapeDtypeStruct((8, 4 * hidden), F32)],
        scratch_shapes=[
            pltpu.VMEM((rows, hidden), F32),
            pltpu.VMEM(w_t.shape, BF16),
            pltpu.VMEM((2, rows, 4 * hidden), BF16),
            pltpu.SemaphoreType.DMA((steps,)),
        ],
        compiler_params=pltpu.CompilerParams(dimension_semantics=("arbitrary",), vmem_limit_bytes=VMEM_BYTES),
        cost_estimate=pl.CostEstimate(flops=2 * total * hidden * 4 * hidden, bytes_accessed=4 * hidden * hidden * 4, transcendentals=0),
    )(e, acts, acts, w_t)
    return outs[0], outs[1:-1], outs[-1]


def weight_kernel(rows, m_blk, aliased, core_ref, u_ref, h_ref, dz_ref, *refs):
    refs = list(refs)
    if aliased:
        refs.pop(0)
    out_ref, send_ref, later = refs
    d, n_dev = pl.program_id(1), pl.num_programs(1)
    hidden, total = u_ref.shape[1:]
    later[pl.ds(0, total - rows), :] = dz_ref[0, rows:, :]
    later[pl.ds(total - rows, rows), :] = jnp.zeros((rows, later.shape[1]), BF16)

    def share(m0):
        if m0 < hidden:
            total_sum = dot(u_ref[0, pl.ds(m0, m_blk), :], dz_ref[0])
        else:
            total_sum = dot(h_ref[0, pl.ds(m0 - hidden, m_blk), :], later[...])
        return total_sum.astype(BF16).astype(F32)

    @pl.when(d < n_dev - 1)
    def _():
        for m0 in range(0, 2 * hidden, m_blk):
            at = pl.ds(m0, m_blk)
            out_ref[0, at, :] = jnp.where(d == 0, 0.0, out_ref[0, at, :]) + share(m0)

    @pl.when(d == n_dev - 1)
    def _():
        for m0 in range(0, 2 * hidden, m_blk):
            at = pl.ds(m0, m_blk)
            low = (out_ref[0, at, :] + share(m0)).astype(BF16)
            out_ref[0, at, :] = low.astype(F32)
            send_ref[0, at, :] = low


def weight_grads(layer, col, n_blk, core, u_all, h_all, dz_all, rows, out_shape, dw):
    n_dev, hidden, total = u_all.shape
    n_col = dz_all.shape[2] // n_blk // 2
    whole = pl.BlockSpec((1, hidden, total), lambda j, d, c: (d, 0, 0))
    in_specs = [whole, whole, pl.BlockSpec((1, total, n_blk), lambda j, d, c: (d, 0, 2 * j + c[0]))]
    args = [core, u_all, h_all, dz_all]
    aliases = {}
    if dw is not None:
        in_specs.append(pl.BlockSpec(memory_space=pl.ANY))
        aliases = {len(args): 0}
        args.append(dw)
    return pl.pallas_call(
        functools.partial(weight_kernel, rows, hidden // 4, dw is not None),
        grid_spec=pltpu.PrefetchScalarGridSpec(
            num_scalar_prefetch=1,
            grid=(n_col, n_dev),
            in_specs=in_specs,
            out_specs=[
                pl.BlockSpec((1, 2 * hidden, n_blk), lambda j, d, c: (layer, 0, col // n_blk + 2 * j + c[0])),
                pl.BlockSpec((1, 2 * hidden, n_blk), lambda j, d, c: (j, 0, 0)),
            ],
            scratch_shapes=[pltpu.VMEM((total, n_blk), BF16)],
        ),
        out_shape=[out_shape, jax.ShapeDtypeStruct((n_col, 2 * hidden, n_blk), BF16)],
        input_output_aliases=aliases,
        compiler_params=pltpu.CompilerParams(dimension_semantics=("arbitrary", "arbitrary"), vmem_limit_bytes=VMEM_BYTES),
        cost_estimate=pl.CostEstimate(flops=2 * n_dev * total * 2 * hidden * n_col * n_blk, bytes_accessed=n_col * 48 * 2**20, transcendentals=0),
    )(*args)


def widen_kernel(core_ref, recv_ref, dw_ref, out_ref):
    out_ref[...] = recv_ref[...].astype(F32)


def widen(layer, col, core, recv, dw):
    n_col, tall, n_blk = recv.shape
    m_blk = tall // 4
    return pl.pallas_call(
        widen_kernel,
        grid_spec=pltpu.PrefetchScalarGridSpec(
            num_scalar_prefetch=1,
            grid=(n_col, tall // m_blk),
            in_specs=[pl.BlockSpec((1, m_blk, n_blk), lambda j, m, c: (j, m, 0)), pl.BlockSpec(memory_space=pl.ANY)],
            out_specs=pl.BlockSpec((1, m_blk, n_blk), lambda j, m, c: (layer, m, col // n_blk + 2 * j + 1 - c[0])),
        ),
        out_shape=jax.ShapeDtypeStruct(dw.shape, F32),
        input_output_aliases={2: 0},
        compiler_params=pltpu.CompilerParams(dimension_semantics=("arbitrary", "arbitrary")),
        cost_estimate=pl.CostEstimate(flops=n_col * tall * n_blk, bytes_accessed=6 * n_col * tall * n_blk, transcendentals=0),
    )(core, recv, dw)


def transpose_kernel(a_ref, out_ref):
    out_ref[...] = a_ref[...].T


def transpose(a):
    tall, wide = a.shape
    blk = wide // 8
    return pl.pallas_call(
        transpose_kernel,
        grid=(8,),
        in_specs=[pl.BlockSpec((tall, blk), lambda k: (0, k))],
        out_specs=pl.BlockSpec((blk, tall), lambda k: (k, 0)),
        out_shape=jax.ShapeDtypeStruct((wide, tall), a.dtype),
        cost_estimate=pl.CostEstimate(flops=tall * wide, bytes_accessed=4 * tall * wide, transcendentals=0),
        name="transpose_x",
    )(a)


def batch_major_kernel(a_ref, out_ref):
    out_ref[...] = jnp.swapaxes(a_ref[...], 0, 1)


def batch_major(a):
    steps, rows, hidden = a.shape
    blk = hidden // 8
    return pl.pallas_call(
        batch_major_kernel,
        grid=(8,),
        in_specs=[pl.BlockSpec((steps, rows, blk), lambda k: (0, 0, k))],
        out_specs=pl.BlockSpec((rows, steps, blk), lambda k: (0, 0, k)),
        out_shape=jax.ShapeDtypeStruct((rows, steps, hidden), a.dtype),
        cost_estimate=pl.CostEstimate(flops=steps * rows * hidden, bytes_accessed=8 * steps * rows * hidden, transcendentals=0),
        name="batch_major",
    )(a)


def solution(mesh):
    axes = ("replica", "data")
    n_data = mesh.shape["data"]
    swap = [(k, k ^ 1) for k in range(n_data)]

    def gather(a):
        return lax.all_gather(a, axes, axis=0, tiled=False)

    def body(x_loc, dy_loc, w_stack, b_stack):
        rows, steps, hidden = x_loc.shape
        total = rows * steps
        core = lax.rem(lax.axis_index("data"), 2).astype(jnp.int32)[None]
        dw_shape = jax.ShapeDtypeStruct(w_stack.shape, F32)
        widths = {layer: [int(hidden * w) for w in PIECES[layer]] for layer in PIECES}

        u_0 = jnp.swapaxes(x_loc, 0, 1).reshape(total, hidden)
        e_1 = jnp.swapaxes(dy_loc, 0, 1).reshape(total, hidden)
        x_all = gather(transpose(u_0))
        acts_0, u_1, h0_t, w_t0 = forward(0, u_0, w_stack, b_stack, rows, steps)
        h0_all = gather(h0_t)
        acts_1, _, h1_t, w_t1 = forward(1, u_1, w_stack, b_stack, rows, steps)
        h1_all = gather(h1_t)

        dz_1, pieces_1, db_1 = backward(1, e_1, acts_1, w_t1, rows, widths[1])
        all_1 = [gather(a) for a in pieces_1]
        e_0 = jnp.einsum("rg,hg->rh", dz_1, w_stack[1, :hidden], preferred_element_type=F32)
        dz_0, pieces_0, db_0 = backward(0, e_0, acts_0, w_t0, rows, widths[0])
        all_0 = [gather(a) for a in pieces_0]
        dx = jnp.einsum("rg,hg->rh", dz_0, w_stack[0, :hidden], preferred_element_type=F32)
        dx = batch_major(dx.reshape(steps, rows, hidden))
        db = [lax.psum(jnp.sum(a, axis=0).astype(BF16), axes).astype(F32) for a in (db_0, db_1)]
        all_1[0], dx, *db = lax.optimization_barrier((all_1[0], dx, *db))

        jobs = []
        for layer, gathered, u_all, h_all in ((1, all_1, h0_all, h1_all), (0, all_0, x_all, h0_all)):
            col = 0
            for width, dz_all in zip(widths[layer], gathered):
                jobs.append((layer, col, u_all, h_all, dz_all))
                col += width
        dw, waiting = None, []
        for layer, col, u_all, h_all, dz_all in jobs:
            dw, own = weight_grads(layer, col, hidden // 4, core, u_all, h_all, dz_all, rows, dw_shape, dw)
            waiting.append((layer, col, core, lax.ppermute(own, "data", swap)))
            if len(waiting) == 2:
                for other in waiting:
                    dw = widen(*other, dw)
                waiting = []
        return dw, jnp.stack(db), dx

    return jax.shard_map(body, mesh=mesh, in_specs=(P(axes), P(axes), P(), P()), out_specs=(P(), P(), P(axes)), check_vma=False)
```

```python
import functools

import jax
import jax.numpy as jnp
from jax import lax
from jax.experimental import pallas as pl
from jax.experimental.pallas import tpu as pltpu
from jax.sharding import PartitionSpec as P


VMEM_BYTES = 67043328
BF16, F32 = jnp.bfloat16, jnp.float32
REPEAT = 4
PIECES = {1: (2, 2), 0: (1.5, 1, 1, 0.5)}


def dot(a, b):
    return jnp.dot(a, b, preferred_element_type=F32)


def repeated_dot(a, b, repeat):
    rows = a.shape[0]
    many = dot(jnp.concatenate([a] * repeat, axis=0), b)
    out = many[:rows]
    for k in range(1, repeat):
        out = jnp.maximum(out, many[k * rows : (k + 1) * rows])
    return out


def forward_kernel(layer, rows, steps, in_blk, n_blk, repeat, u_hbm, win_ref, b_ref, w_hbm, acts_ref, h_hbm, ht_hbm, wt_hbm, wrec, zin, uh, c_scr, wt_buf, ht_buf, sem_w, sem_u, sem_o, sem_h):
    hidden = uh.shape[1]
    n_in = 4 * hidden // in_blk
    cut = hidden // steps
    i = pl.program_id(0)
    part = hidden // 8

    w_part = hidden // n_in

    def w_copy(k):
        at = pl.multiple_of(k * w_part, w_part)
        return pltpu.make_async_copy(w_hbm.at[layer, pl.ds(hidden + at, w_part)], wrec.at[pl.ds(at, w_part)], sem_w.at[k])

    def wt_copy(t):
        slot = lax.rem(t, 2)
        return pltpu.make_async_copy(wt_buf.at[slot], wt_hbm.at[t], sem_o.at[slot])

    def ht_copy(k):
        slot = k % 2
        return pltpu.make_async_copy(ht_buf.at[slot], ht_hbm.at[pl.ds(k * part, part)], sem_h.at[slot])

    @pl.when(i == 0)
    def _():
        u_copy = pltpu.make_async_copy(u_hbm, uh, sem_u)
        u_copy.start()
        u_copy.wait()

    @pl.when(i < n_in)
    def _():
        w_copy(i).start()
        zin[:, pl.ds(pl.multiple_of(i * in_blk, in_blk), in_blk)] = dot(uh[...], win_ref[0]) + b_ref[...]

    def step(t, first):
        now = pl.ds(pl.multiple_of(t * rows, rows), rows)
        wt_buf[lax.rem(t, 2)] = wrec[pl.ds(pl.multiple_of(t * cut, cut), cut), :].T
        h_prev = None if first else uh[pl.ds(pl.multiple_of((t - 1) * rows, rows), rows), :]
        for n0 in range(0, hidden, n_blk):
            cols = pl.ds(n0, n_blk)
            z = []
            for g in range(4):
                gcols = pl.ds(g * hidden + n0, n_blk)
                zg = zin[now, gcols]
                z.append(zg if first else zg + repeated_dot(h_prev, wrec[:, gcols], repeat))
            gate_i, gate_f, gate_g, gate_o = jax.nn.sigmoid(z[0]), jax.nn.sigmoid(z[1]), jnp.tanh(z[2]), jax.nn.sigmoid(z[3])
            c_new = gate_i * gate_g if first else gate_f * c_scr[:, cols] + gate_i * gate_g
            tanh_c = jnp.tanh(c_new)
            c_scr[:, cols] = c_new
            uh[now, cols] = (gate_o * tanh_c).astype(BF16)
            for k, a in enumerate((gate_i, gate_f, gate_g, gate_o, tanh_c, c_new)):
                acts_ref[k, :, cols] = a

    @pl.when(i == n_in)
    def _():
        for k in range(n_in):
            w_copy(k).wait()
        step(i - n_in, True)
        wt_copy(i - n_in).start()

    @pl.when(i > n_in)
    def _():
        t = i - n_in

        @pl.when(t > 1)
        def _():
            wt_copy(t - 2).wait()

        step(t, False)
        wt_copy(t).start()

    @pl.when(i == n_in + steps - 1)
    def _():
        h_copy = pltpu.make_async_copy(uh, h_hbm, sem_u)
        h_copy.start()
        for k in range(8):
            if k >= 2:
                ht_copy(k - 2).wait()
            ht_buf[k % 2] = uh[:, pl.ds(k * part, part)].T
            ht_copy(k).start()
        wt_copy(steps - 2).wait()
        wt_copy(steps - 1).wait()
        h_copy.wait()
        for k in range(6, 8):
            ht_copy(k).wait()


def forward(layer, u, w_stack, b_stack, rows, steps):
    total, hidden = u.shape
    in_blk, n_blk = hidden // 4, hidden // 4
    n_in = 4 * hidden // in_blk
    t_of = lambda i: jnp.maximum(i - n_in, 0)
    k_of = lambda i: jnp.minimum(i, n_in - 1)
    return pl.pallas_call(
        functools.partial(forward_kernel, layer, rows, steps, in_blk, n_blk, REPEAT),
        grid=(n_in + steps,),
        in_specs=[
            pl.BlockSpec(memory_space=pl.ANY),
            pl.BlockSpec((1, hidden, in_blk), lambda i: (layer, 0, k_of(i))),
            pl.BlockSpec((1, in_blk), lambda i: (0, k_of(i))),
            pl.BlockSpec(memory_space=pl.ANY),
        ],
        out_specs=[
            pl.BlockSpec((6, rows, hidden), lambda i: (0, t_of(i), 0)),
            pl.BlockSpec(memory_space=pl.ANY),
            pl.BlockSpec(memory_space=pl.ANY),
            pl.BlockSpec(memory_space=pl.ANY),
        ],
        out_shape=[
            jax.ShapeDtypeStruct((6, total, hidden), F32),
            jax.ShapeDtypeStruct((total, hidden), BF16),
            jax.ShapeDtypeStruct((hidden, total), BF16),
            jax.ShapeDtypeStruct((steps, 4 * hidden, hidden // steps), BF16),
        ],
        scratch_shapes=[
            pltpu.VMEM((hidden, 4 * hidden), BF16),
            pltpu.VMEM((total, 4 * hidden), F32),
            pltpu.VMEM((total, hidden), BF16),
            pltpu.VMEM((rows, hidden), F32),
            pltpu.VMEM((2, 4 * hidden, hidden // steps), BF16),
            pltpu.VMEM((2, hidden // 8, total), BF16),
            pltpu.SemaphoreType.DMA((n_in,)),
            pltpu.SemaphoreType.DMA,
            pltpu.SemaphoreType.DMA((2,)),
            pltpu.SemaphoreType.DMA((2,)),
        ],
        compiler_params=pltpu.CompilerParams(dimension_semantics=("arbitrary",), vmem_limit_bytes=VMEM_BYTES),
        cost_estimate=pl.CostEstimate(flops=4 * total * hidden * 4 * hidden, bytes_accessed=4 * hidden * hidden * 4 * 3, transcendentals=0),
    )(u, w_stack, b_stack[layer][None], w_stack)


def backward_kernel(rows, n_steps, widths, n_blk, repeat, e_ref, acts_ref, cprev_ref, wt_hbm, dz_ref, *refs):
    piece_refs = refs[: len(widths)]
    db_ref, fdc, wt, dz_scr, sem_w = refs[len(widths) :]
    starts = [sum(widths[:k]) for k in range(len(widths))]
    hidden = fdc.shape[1]
    n_slab, _, cut = wt.shape
    s = pl.program_id(0)
    t = n_steps - 1 - s

    def w_copy(k):
        return pltpu.make_async_copy(wt_hbm.at[k], wt.at[k], sem_w.at[k])

    def step(first):
        new, old = lax.rem(s, 2), lax.rem(s + 1, 2)
        later = None if first else dz_scr[old]
        for n0 in range(0, hidden, n_blk):
            cols = pl.ds(n0, n_blk)
            gate_i, gate_f, gate_g, gate_o, tanh_c = (acts_ref[k, :, cols] for k in range(5))
            c_prev = jnp.where(t > 0, cprev_ref[0, :, cols], 0.0)
            dh = e_ref[:, cols]
            if not first:
                w_cols = jnp.concatenate([wt[n0 // cut + k] for k in range(n_blk // cut)], axis=1)
                dh = dh + repeated_dot(later, w_cols, repeat)
            dc = dh * gate_o * (1.0 - tanh_c * tanh_c)
            if not first:
                dc = fdc[:, cols] + dc
            fdc[:, cols] = dc * gate_f
            dz = (
                dc * gate_g * gate_i * (1.0 - gate_i),
                dc * c_prev * gate_f * (1.0 - gate_f),
                dc * gate_i * (1.0 - gate_g * gate_g),
                dh * tanh_c * gate_o * (1.0 - gate_o),
            )
            for k in range(4):
                at = k * hidden + n0
                gcols = pl.ds(at, n_blk)
                low = dz[k].astype(BF16)
                dz_scr[new, :, gcols] = low
                dz_ref[:, gcols] = low
                for ref, start in zip(piece_refs, starts):
                    if start <= at < start + ref.shape[1]:
                        ref[:, pl.ds(at - start, n_blk)] = low
                part_sum = dz[k][0:8]
                for q in range(8, rows, 8):
                    part_sum = part_sum + dz[k][q : q + 8]
                if first:
                    db_ref[:, gcols] = part_sum
                else:
                    db_ref[:, gcols] += part_sum

    @pl.when(s == 0)
    def _():
        for k in range(n_slab):
            w_copy(k).start()
        step(True)
        for k in range(n_slab):
            w_copy(k).wait()

    @pl.when(s > 0)
    def _():
        step(False)


def backward(e, acts, w_t, rows, widths):
    total, hidden = acts.shape[1:]
    steps = total // rows
    back = lambda s: (steps - 1 - s, 0)
    outs = pl.pallas_call(
        functools.partial(backward_kernel, rows, steps, widths, hidden // 8, REPEAT),
        grid=(steps,),
        in_specs=[
            pl.BlockSpec((rows, hidden), back),
            pl.BlockSpec((6, rows, hidden), lambda s: (0, steps - 1 - s, 0)),
            pl.BlockSpec((1, rows, hidden), lambda s: (5, jnp.maximum(steps - 2 - s, 0), 0)),
            pl.BlockSpec(memory_space=pl.ANY),
        ],
        out_specs=[pl.BlockSpec((rows, w), back) for w in (4 * hidden, *widths)] + [pl.BlockSpec((8, 4 * hidden), lambda s: (0, 0))],
        out_shape=[jax.ShapeDtypeStruct((total, w), BF16) for w in (4 * hidden, *widths)] + [jax.ShapeDtypeStruct((8, 4 * hidden), F32)],
        scratch_shapes=[
            pltpu.VMEM((rows, hidden), F32),
            pltpu.VMEM(w_t.shape, BF16),
            pltpu.VMEM((2, rows, 4 * hidden), BF16),
            pltpu.SemaphoreType.DMA((steps,)),
        ],
        compiler_params=pltpu.CompilerParams(dimension_semantics=("arbitrary",), vmem_limit_bytes=VMEM_BYTES),
        cost_estimate=pl.CostEstimate(flops=2 * total * hidden * 4 * hidden, bytes_accessed=4 * hidden * hidden * 4, transcendentals=0),
    )(e, acts, acts, w_t)
    return outs[0], outs[1:-1], outs[-1]


def weight_kernel(rows, m_blk, aliased, core_ref, u_ref, h_ref, dz_ref, *refs):
    refs = list(refs)
    if aliased:
        refs.pop(0)
    out_ref, send_ref, later = refs
    d, n_dev = pl.program_id(1), pl.num_programs(1)
    hidden, total = u_ref.shape[1:]
    later[pl.ds(0, total - rows), :] = dz_ref[0, rows:, :]
    later[pl.ds(total - rows, rows), :] = jnp.zeros((rows, later.shape[1]), BF16)

    def share(m0):
        if m0 < hidden:
            total_sum = dot(u_ref[0, pl.ds(m0, m_blk), :], dz_ref[0])
        else:
            total_sum = dot(h_ref[0, pl.ds(m0 - hidden, m_blk), :], later[...])
        return total_sum.astype(BF16).astype(F32)

    @pl.when(d < n_dev - 1)
    def _():
        for m0 in range(0, 2 * hidden, m_blk):
            at = pl.ds(m0, m_blk)
            out_ref[0, at, :] = jnp.where(d == 0, 0.0, out_ref[0, at, :]) + share(m0)

    @pl.when(d == n_dev - 1)
    def _():
        for m0 in range(0, 2 * hidden, m_blk):
            at = pl.ds(m0, m_blk)
            low = (out_ref[0, at, :] + share(m0)).astype(BF16)
            out_ref[0, at, :] = low.astype(F32)
            send_ref[0, at, :] = low


def weight_grads(layer, col, n_blk, core, u_all, h_all, dz_all, rows, out_shape, dw):
    n_dev, hidden, total = u_all.shape
    n_col = dz_all.shape[2] // n_blk // 2
    whole = pl.BlockSpec((1, hidden, total), lambda j, d, c: (d, 0, 0))
    in_specs = [whole, whole, pl.BlockSpec((1, total, n_blk), lambda j, d, c: (d, 0, 2 * j + c[0]))]
    args = [core, u_all, h_all, dz_all]
    aliases = {}
    if dw is not None:
        in_specs.append(pl.BlockSpec(memory_space=pl.ANY))
        aliases = {len(args): 0}
        args.append(dw)
    return pl.pallas_call(
        functools.partial(weight_kernel, rows, hidden // 4, dw is not None),
        grid_spec=pltpu.PrefetchScalarGridSpec(
            num_scalar_prefetch=1,
            grid=(n_col, n_dev),
            in_specs=in_specs,
            out_specs=[
                pl.BlockSpec((1, 2 * hidden, n_blk), lambda j, d, c: (layer, 0, col // n_blk + 2 * j + c[0])),
                pl.BlockSpec((1, 2 * hidden, n_blk), lambda j, d, c: (j, 0, 0)),
            ],
            scratch_shapes=[pltpu.VMEM((total, n_blk), BF16)],
        ),
        out_shape=[out_shape, jax.ShapeDtypeStruct((n_col, 2 * hidden, n_blk), BF16)],
        input_output_aliases=aliases,
        compiler_params=pltpu.CompilerParams(dimension_semantics=("arbitrary", "arbitrary"), vmem_limit_bytes=VMEM_BYTES),
        cost_estimate=pl.CostEstimate(flops=2 * n_dev * total * 2 * hidden * n_col * n_blk, bytes_accessed=n_col * 48 * 2**20, transcendentals=0),
    )(*args)


def widen_kernel(core_ref, recv_ref, dw_ref, out_ref):
    out_ref[...] = recv_ref[...].astype(F32)


def widen(layer, col, core, recv, dw):
    n_col, tall, n_blk = recv.shape
    m_blk = tall // 4
    return pl.pallas_call(
        widen_kernel,
        grid_spec=pltpu.PrefetchScalarGridSpec(
            num_scalar_prefetch=1,
            grid=(n_col, tall // m_blk),
            in_specs=[pl.BlockSpec((1, m_blk, n_blk), lambda j, m, c: (j, m, 0)), pl.BlockSpec(memory_space=pl.ANY)],
            out_specs=pl.BlockSpec((1, m_blk, n_blk), lambda j, m, c: (layer, m, col // n_blk + 2 * j + 1 - c[0])),
        ),
        out_shape=jax.ShapeDtypeStruct(dw.shape, F32),
        input_output_aliases={2: 0},
        compiler_params=pltpu.CompilerParams(dimension_semantics=("arbitrary", "arbitrary")),
        cost_estimate=pl.CostEstimate(flops=n_col * tall * n_blk, bytes_accessed=6 * n_col * tall * n_blk, transcendentals=0),
    )(core, recv, dw)


def transpose_kernel(a_ref, out_ref):
    out_ref[...] = a_ref[...].T


def transpose(a):
    tall, wide = a.shape
    blk = wide // 8
    return pl.pallas_call(
        transpose_kernel,
        grid=(8,),
        in_specs=[pl.BlockSpec((tall, blk), lambda k: (0, k))],
        out_specs=pl.BlockSpec((blk, tall), lambda k: (k, 0)),
        out_shape=jax.ShapeDtypeStruct((wide, tall), a.dtype),
        cost_estimate=pl.CostEstimate(flops=tall * wide, bytes_accessed=4 * tall * wide, transcendentals=0),
        name="transpose_x",
    )(a)


def batch_major_kernel(a_ref, out_ref):
    out_ref[...] = jnp.swapaxes(a_ref[...], 0, 1)


def batch_major(a):
    steps, rows, hidden = a.shape
    blk = hidden // 8
    return pl.pallas_call(
        batch_major_kernel,
        grid=(8,),
        in_specs=[pl.BlockSpec((steps, rows, blk), lambda k: (0, 0, k))],
        out_specs=pl.BlockSpec((rows, steps, blk), lambda k: (0, 0, k)),
        out_shape=jax.ShapeDtypeStruct((rows, steps, hidden), a.dtype),
        cost_estimate=pl.CostEstimate(flops=steps * rows * hidden, bytes_accessed=8 * steps * rows * hidden, transcendentals=0),
        name="batch_major",
    )(a)


def solution(mesh):
    axes = ("replica", "data")
    n_data = mesh.shape["data"]
    swap = [(k, k ^ 1) for k in range(n_data)]

    def gather(a):
        return lax.all_gather(a, axes, axis=0, tiled=False)

    def body(x_loc, dy_loc, w_stack, b_stack):
        rows, steps, hidden = x_loc.shape
        total = rows * steps
        core = lax.rem(lax.axis_index("data"), 2).astype(jnp.int32)[None]
        dw_shape = jax.ShapeDtypeStruct(w_stack.shape, F32)
        widths = {layer: [int(hidden * w) for w in PIECES[layer]] for layer in PIECES}

        u_0 = jnp.swapaxes(x_loc, 0, 1).reshape(total, hidden)
        e_1 = jnp.swapaxes(dy_loc, 0, 1).reshape(total, hidden)
        x_all = gather(transpose(u_0))
        acts_0, u_1, h0_t, w_t0 = forward(0, u_0, w_stack, b_stack, rows, steps)
        h0_all = gather(h0_t)
        acts_1, _, h1_t, w_t1 = forward(1, u_1, w_stack, b_stack, rows, steps)
        h1_all = gather(h1_t)

        dz_1, pieces_1, db_1 = backward(e_1, acts_1, w_t1, rows, widths[1])
        all_1 = [gather(a) for a in pieces_1]
        e_0 = jnp.einsum("rg,hg->rh", dz_1, w_stack[1, :hidden], preferred_element_type=F32)
        dz_0, pieces_0, db_0 = backward(e_0, acts_0, w_t0, rows, widths[0])
        all_0 = [gather(a) for a in pieces_0]
        dx = jnp.einsum("rg,hg->rh", dz_0, w_stack[0, :hidden], preferred_element_type=F32)
        dx = batch_major(dx.reshape(steps, rows, hidden))
        db = [lax.psum(jnp.sum(a, axis=0).astype(BF16), axes).astype(F32) for a in (db_0, db_1)]
        all_1[0], dx, *db = lax.optimization_barrier((all_1[0], dx, *db))

        jobs = []
        for layer, gathered, u_all, h_all in ((1, all_1, h0_all, h1_all), (0, all_0, x_all, h0_all)):
            col = 0
            for width, dz_all in zip(widths[layer], gathered):
                jobs.append((layer, col, u_all, h_all, dz_all))
                col += width
        dw, waiting = None, []
        for layer, col, u_all, h_all, dz_all in jobs:
            dw, own = weight_grads(layer, col, hidden // 4, core, u_all, h_all, dz_all, rows, dw_shape, dw)
            waiting.append((layer, col, core, lax.ppermute(own, "data", swap)))
            if len(waiting) == 2:
                for other in waiting:
                    dw = widen(*other, dw)
                waiting = []
        return dw, jnp.stack(db), dx

    return jax.shard_map(body, mesh=mesh, in_specs=(P(axes), P(axes), P(), P()), out_specs=(P(), P(), P(axes)), check_vma=False)
```
